32 devices in a mesh: nest: 4 (over y, x), tile: 8 (over z, core).
Axes of the slice: x: 2, y: 2, z: 4, core: 2. Of those that a mesh axis runs over, the one named last changes fastest.
Arguments:
- child_fields: float32 [4, 32, 192, 384], P('nest', None, 'tile'), may hold values from -18 to 18
- row_weights: float32 [8, 24], replicated
- col_weights: float32 [384, 128], replicated
- nest_offsets: int32 [4, 2], replicated, may hold values from 0 to 960, as said below
- priority: int32 [128, 1024], P('tile', 'nest'), may hold values from -1 to 3, as said below
- parent_old: float32 [32, 128, 1024], P(None, 'tile', 'nest'), may hold values from -6 to 6
- smooth_rate: float32 [32], replicated, may hold values from 0.03 to 0.22
Outputs:
- parent_new: float32 [32, 128, 1024], P(None, 'tile', 'nest')
The draws below stay inside these ranges and needn't reach their ends.
Inputs may be any that keep to these rules, and one draw needn't show every extreme that they name: nest_offsets[n, 0] lies in 0 .. 960 and nest_offsets[n, 1] in 0 .. 127. priority[x, y] is -1 or a nest n with nest_offsets[n, 0] <= y < nest_offsets[n, 0] + 64.
All inputs are finite; a program needn't handle non-finite values.
Results may differ from the reference program's by a relative error of at most 0.000058.
Values sent between devices are 32-bit elements; how exact they have to be, the bound alone decides.
A program may use at most 128 MiB of HBM per device.

```python
import math
import jax
import jax.numpy as jnp
from jax import lax

CROW = 24
FL = 32
PRD = 8
PCOLS = 128
CW = 384
CROWS_ALL = 192
NR = 64
PROWS_ALL = 1024
NESTS = 4


def nest_layout(key):
    key_top, key_left, key_score, key_skip, key_order = jax.random.split(jax.random.fold_in(key, 7), 5)
    top_rows = jax.random.randint(key_top, (NESTS,), 0, PROWS_ALL - NR + 1)
    left_cols = jax.random.randint(key_left, (NESTS,), 0, PCOLS)
    order = jax.random.permutation(key_order, NESTS)
    top_rows = top_rows.at[order[0]].set(PROWS_ALL - NR)
    top_rows = top_rows.at[order[1 % NESTS]].set(0)
    left_cols = left_cols.at[order[2 % NESTS]].set(PCOLS - 1)
    left_cols = left_cols.at[order[3 % NESTS]].set(0)
    row_ids = jnp.arange(PROWS_ALL)
    covered = (row_ids[None, :] >= top_rows[:, None]) & (row_ids[None, :] < top_rows[:, None] + NR)
    scores = jax.random.randint(key_score, (NESTS, PCOLS, PROWS_ALL), 0, 1000) * NESTS + jnp.arange(NESTS)[:, None, None]
    scores = jnp.where(covered[:, None, :], scores, -1)
    chosen = jnp.argmax(scores, axis=0).astype(jnp.int32)
    any_cover = jnp.any(covered, axis=0)
    skipped = jax.random.randint(key_skip, (PCOLS, PROWS_ALL), 0, 4) == 0
    priority_map = jnp.where(any_cover[None, :] & jnp.logical_not(skipped), chosen, -1)
    offsets = jnp.stack([top_rows, left_cols], axis=1)
    return (offsets.astype(jnp.int32), priority_map.astype(jnp.int32))


def draw_nest_offsets(key, part):
    return nest_layout(key)[0]


def draw_priority(key, part):
    return nest_layout(key)[1]


def draw_row_weights(key, part):
    tap_weights = jax.random.uniform(key, (PRD, 3), jnp.float32, 0.5, 1.5)
    tap_weights = tap_weights / jnp.sum(tap_weights, axis=1, keepdims=True)
    col_ids = jnp.arange(CROW)
    parent_ids = jnp.arange(PRD)
    matrix = jnp.zeros((PRD, CROW), jnp.float32)
    for member in range(3):
        matrix = matrix + tap_weights[:, member:member + 1] * (col_ids[None, :] == 3 * parent_ids[:, None] + member).astype(jnp.float32)
    return matrix


def draw_col_weights(key, part):
    key_inner, key_outer = jax.random.split(key)
    inner = jax.random.uniform(key_inner, (PCOLS, 3), jnp.float32, 0.5, 1.5)
    outer = jax.random.uniform(key_outer, (PCOLS, 2), jnp.float32, 0.1, 0.5)
    tap_weights = jnp.concatenate([outer[:, :1], inner, outer[:, 1:]], axis=1)
    tap_weights = tap_weights / jnp.sum(tap_weights, axis=1, keepdims=True)
    child_ids = jnp.arange(CW)
    parent_ids = jnp.arange(PCOLS)
    matrix = jnp.zeros((CW, PCOLS), jnp.float32)
    for member in range(5):
        target = (3 * parent_ids + member - 1) % CW
        matrix = matrix + tap_weights[None, :, member] * (child_ids[:, None] == target[None, :]).astype(jnp.float32)
    return matrix


def block_levels(key, extent, pieces, smallest, largest):
    loudness, own = 1.0, jax.random.fold_in(key, 6)
    for dim, shards_of in pieces:
        heights = jnp.exp(jax.random.uniform(jax.random.fold_in(own, dim), (shards_of,), jnp.float32, smallest / len(pieces), largest / len(pieces)))
        loudness = loudness * jnp.repeat(heights, extent[dim] // shards_of).reshape([-1 if axis == dim else 1 for axis in range(len(extent))])
    return loudness


def normal_values(key, dims, deviation, limit, cuts=(), kind=jnp.bfloat16):
    gain = block_levels(key, dims, cuts, -0.22, 0.18) if cuts else 1.0
    entries = jax.random.normal(key, dims, jnp.float32) * deviation * gain
    return jnp.minimum(jnp.maximum(entries, -limit), limit).astype(kind)


def setup_inputs(seed: int = 0) -> dict:
    key_list = jax.random.split(jax.random.key(seed), 8)
    child_fields = normal_values(key_list[0], (NESTS, FL, CROWS_ALL, CW), 3.0, 18.0, ((0, 4), (2, 8)), jnp.float32)
    row_weights = draw_row_weights(jax.random.fold_in(key_list[7], 71), 0)
    col_weights = draw_col_weights(jax.random.fold_in(key_list[7], 71), 0)
    nest_offsets = draw_nest_offsets(jax.random.fold_in(key_list[7], 71), 0)
    priority = draw_priority(jax.random.fold_in(key_list[7], 71), 0)
    parent_old = normal_values(key_list[5], (FL, PCOLS, PROWS_ALL), 1.0, 6.0, ((1, 8), (2, 4)), jnp.float32)
    smooth_rate = jnp.clip(jnp.exp(jax.random.uniform(key_list[6], (FL,), jnp.float32, math.log(0.03), math.log(0.22))), 0.03, 0.22)
    return {"child_fields": child_fields, "row_weights": row_weights, "col_weights": col_weights, "nest_offsets": nest_offsets, "priority": priority, "parent_old": parent_old, "smooth_rate": smooth_rate}


def reference(child_fields, row_weights, col_weights, nest_offsets, priority, parent_old, smooth_rate):
    nest_count, planes, crows_all, child_cols = child_fields.shape
    cell_rows, child_rows = row_weights.shape
    row_blocks = crows_all // child_rows
    nrows = row_blocks * cell_rows

    def restrict_one(child_block):
        grouped = child_block.reshape(planes, row_blocks, child_rows, child_cols)
        thinned = jnp.einsum('pr,ftrc->ftpc', row_weights, grouped, precision=lax.Precision.HIGHEST)
        thinned = thinned.reshape(planes, nrows, child_cols)
        return jnp.einsum('fyc,cx->fxy', thinned, col_weights, precision=lax.Precision.HIGHEST)

    restricted = lax.map(restrict_one, child_fields)
    merged = parent_old
    for nest_num in range(nest_count):
        rolled = jnp.roll(restricted[nest_num], nest_offsets[nest_num, 1], axis=1)
        placed = lax.dynamic_update_slice(jnp.zeros_like(parent_old), rolled,
                                          (jnp.int32(0), jnp.int32(0), nest_offsets[nest_num, 0].astype(jnp.int32)))
        merged = jnp.where((priority == nest_num)[None], placed, merged)
    east_side = jnp.roll(merged, -1, axis=1)
    west_side = jnp.roll(merged, 1, axis=1)
    padded = jnp.concatenate([merged[:, :, :1], merged, merged[:, :, -1:]], axis=2)
    north_side = padded[:, :, 2:]
    south_side = padded[:, :, :-2]
    return merged + smooth_rate[:, None, None] * (east_side + west_side + north_side + south_side - 4.0 * merged)
```

```python
import functools

import jax
import jax.numpy as jnp
from jax import lax
from jax.experimental import pallas as pl
from jax.experimental.pallas import tpu as pltpu
from jax.sharding import PartitionSpec as P

MESH = pl.DeviceIdType.MESH
LANES = 128
F32 = jnp.float32
BF16 = jnp.bfloat16


def split(value):
    high = value.astype(BF16)
    return high, (value - high.astype(F32)).astype(BF16)


def dot(a, b):
    return jnp.dot(a, b, preferred_element_type=F32)


def dot3(a, b):
    (ah, al), (bh, bl) = a, b
    return dot(ah, bh) + (dot(ah, bl) + dot(al, bh))


def remote(src, dst, send_sem, recv_sem, where):
    return pltpu.make_async_remote_copy(
        src_ref=src,
        dst_ref=dst,
        send_sem=send_sem,
        recv_sem=recv_sem,
        device_id=where,
        device_id_type=MESH,
    )


def kernel(
    tiles,
    nests,
    offs_ref,
    rate_ref,
    rw_ref,
    prio_ref,
    child_hbm,
    cw_hbm,
    parent_hbm,
    out_hbm,
    child,
    cw,
    merged,
    pieces,
    strips,
    ew_out,
    ew_in,
    ns_out,
    ns_in,
    result,
    child_sem,
    cw_sem,
    parent_sem,
    out_sem,
    a2a_send,
    a2a_recv,
    slab_send,
    slab_recv,
    edge_send,
    edge_recv,
):
    planes, crow, _ = child.shape
    prd = rw_ref.shape[0]
    cols, rows = prio_ref.shape
    per = LANES // cols
    groups = planes // per
    nrows = prd * tiles
    me_n, me_t = lax.axis_index("nest"), lax.axis_index("tile")

    def group(ref, g):
        return ref.at[pl.ds(g * per, per)]

    child_in = [
        pltpu.make_async_copy(group(child_hbm.at[0], g), group(child, g), child_sem.at[g])
        for g in range(groups)
    ]
    cw_in = pltpu.make_async_copy(cw_hbm, cw, cw_sem)
    parent_in = pltpu.make_async_copy(parent_hbm, merged, parent_sem)
    child_in[0].start()
    cw_in.start()
    for g in range(1, groups):
        child_in[g].start()
    parent_in.start()

    barrier = pltpu.get_barrier_semaphore()
    for d in range(1, tiles):
        pl.semaphore_signal(
            barrier, inc=1, device_id={"tile": lax.rem(me_t + d, tiles)}, device_id_type=MESH
        )
    for d in range(1, nests):
        pl.semaphore_signal(
            barrier, inc=1, device_id={"nest": lax.rem(me_n + d, nests)}, device_id_type=MESH
        )

    rw = rw_ref[...]
    spread_rows = lax.broadcasted_iota(jnp.int32, (per * crow, crow), 0)
    spread_cols = lax.broadcasted_iota(jnp.int32, (per * crow, crow), 1)
    spread = jnp.where(lax.rem(spread_rows, crow) == spread_cols, 1.0, 0.0).astype(BF16)
    wide_r = lax.broadcasted_iota(jnp.int32, (per * prd, per * crow), 0)
    wide_c = lax.broadcasted_iota(jnp.int32, (per * prd, per * crow), 1)
    diagonal = wide_r // prd == wide_c // crow
    block_rw = []
    for part in split(rw):
        line = lax.dot_general(
            part, spread, (((1,), (1,)), ((), ())), preferred_element_type=F32
        )
        line = jnp.concatenate([line] * per, axis=0)
        block_rw.append(jnp.where(diagonal, line, 0.0).astype(BF16))

    lane_group = lax.broadcasted_iota(jnp.int32, (prd, LANES), 1) // cols
    left = jnp.int32(0)
    for n in range(nests):
        left = jnp.where(me_n == n, offs_ref[n, 1], left)

    a2a = []
    cw_split = None
    for g in range(groups):
        child_in[g].wait()
        block = child[g * per : (g + 1) * per].reshape(per * crow, child.shape[2])
        thinned = dot3(block_rw, split(block))
        if g == 0:
            cw_in.wait()
            cw_split = split(cw[...])
        restricted = dot3(split(thinned), cw_split)
        restricted = pltpu.roll(restricted, left, 1)
        for t in range(tiles):
            base, off = (t * cols) // LANES * LANES, (t * cols) % LANES
            piece = None
            for j in range(per):
                part = restricted[j * prd : (j + 1) * prd, base : base + LANES]
                shift = (j * cols - off) % LANES
                if shift:
                    part = pltpu.roll(part, shift, 1)
                piece = part if j == 0 else jnp.where(lane_group == j, part, piece)
            pieces[g, t] = piece
        here = pl.ds(pl.multiple_of(me_t * prd, prd), prd)
        strips[me_n, g, here, :] = pieces[g, me_t]
        if g == 0:
            pl.semaphore_wait(barrier, tiles + nests - 2)
        for d in range(1, tiles):
            t = lax.rem(me_t + d, tiles)
            copy = remote(
                pieces.at[g, t],
                strips.at[me_n, g, here, :],
                a2a_send.at[g, t],
                a2a_recv.at[g, me_t],
                {"tile": t},
            )
            copy.start()
            a2a.append(copy)

    slabs = []

    def send_slab(owner, g, to, slot):
        copy = remote(
            strips.at[owner, g],
            strips.at[owner, g],
            slab_send.at[g, slot],
            slab_recv.at[g, owner],
            {"nest": to},
        )
        copy.start()
        slabs.append(copy)

    def wait_slab(owner, g):
        remote(
            strips.at[owner, g],
            strips.at[owner, g],
            slab_send.at[g, 0],
            slab_recv.at[g, owner],
            {"nest": owner},
        ).wait_recv()

    def flip(mask):
        if mask == 1:
            return me_n + 1 - 2 * lax.rem(me_n, 2)
        if mask == 2:
            return lax.rem(me_n + 2, 4)
        return 3 - me_n

    relayed = nests == 4

    def relay(g):
        first, second = (flip(1), flip(2)) if g % 2 == 0 else (flip(2), flip(1))
        wait_slab(first, g)
        send_slab(first, g, second, 2)

    for g in range(groups):
        for d in range(1, tiles):
            t = lax.rem(me_t + d, tiles)
            there = pl.ds(pl.multiple_of(t * prd, prd), prd)
            remote(
                pieces.at[g, t],
                strips.at[me_n, g, there, :],
                a2a_send.at[g, t],
                a2a_recv.at[g, t],
                {"tile": t},
            ).wait_recv()
        if relayed:
            send_slab(me_n, g, flip(1), 0)
            send_slab(me_n, g, flip(2), 1)
            if g:
                relay(g - 1)
        else:
            for d in range(1, nests):
                send_slab(me_n, g, lax.rem(me_n + d, nests), d - 1)
    if relayed:
        relay(groups - 1)

    own_start = me_n * rows
    place_r = lax.rem(lax.broadcasted_iota(jnp.int32, (2 * nrows, rows), 0), nrows)
    place_c = lax.broadcasted_iota(jnp.int32, (2 * nrows, rows), 1)
    prio = prio_ref[...]
    west_t, east_t = lax.rem(me_t + tiles - 1, tiles), lax.rem(me_t + 1, tiles)
    low_n, high_n = lax.rem(me_n + nests - 1, nests), lax.rem(me_n + 1, nests)
    lane = lax.broadcasted_iota(jnp.int32, (cols, LANES), 1)
    places = []
    for n in range(nests):
        hit = place_c - place_r == offs_ref[n, 0] - own_start
        places.append(jnp.where(hit, 1.0, 0.0).astype(BF16))

    edges = []
    parent_in.wait()
    for g in range(groups):
        if relayed:
            first, second = (flip(1), flip(2)) if g % 2 == 0 else (flip(2), flip(1))
            wait_slab(second, g)
            wait_slab(flip(3), g)
        else:
            for d in range(1, nests):
                wait_slab(lax.rem(me_n + d, nests), g)
        now = merged[g * per : (g + 1) * per]
        for n in range(nests):
            slab = jnp.concatenate(split(strips[n, g]), axis=0)
            placed = lax.dot_general(
                slab, places[n], (((0,), (0,)), ((), ())), preferred_element_type=F32
            )
            now = jnp.where((prio == n)[None], placed.reshape(per, cols, rows), now)
        merged[g * per : (g + 1) * per] = now
        low = jnp.zeros((cols, LANES), F32)
        high = jnp.zeros((cols, LANES), F32)
        for j in range(per):
            low = jnp.where(lane == j, now[j, :, :1], low)
            high = jnp.where(lane == j, now[j, :, rows - 1 :], high)
            ew_out[g, 0, j : j + 1] = now[j, :1]
            ew_out[g, 1, j : j + 1] = now[j, cols - 1 :]
        ns_out[g, 0] = low
        ns_out[g, 1] = high
        for side, (source, target, where) in enumerate(
            (
                (ew_out.at[g, 0], ew_in.at[g, 0], {"tile": west_t}),
                (ew_out.at[g, 1], ew_in.at[g, 1], {"tile": east_t}),
                (ns_out.at[g, 0], ns_in.at[g, 0], {"nest": low_n}),
                (ns_out.at[g, 1], ns_in.at[g, 1], {"nest": high_n}),
            )
        ):
            copy = remote(source, target, edge_send.at[g, side], edge_recv.at[g, side], where)
            copy.start()
            edges.append(copy)

    row_lane = lax.broadcasted_iota(jnp.int32, (cols, rows), 1)
    outs = []
    for g in range(groups):
        for side in range(4):
            edges[4 * g + side].wait_recv()
        for j in range(per):
            f = g * per + j
            now = merged[f]
            east = jnp.concatenate([now[1:], ew_in[g, 0, j : j + 1]], axis=0)
            west = jnp.concatenate([ew_in[g, 1, j : j + 1], now[:-1]], axis=0)
            above = jnp.where(me_n == nests - 1, now[:, rows - 1 :], ns_in[g, 0, :, j : j + 1])
            below = jnp.where(me_n == 0, now[:, :1], ns_in[g, 1, :, j : j + 1])
            north = jnp.where(row_lane == rows - 1, above, pltpu.roll(now, rows - 1, 1))
            south = jnp.where(row_lane == 0, below, pltpu.roll(now, 1, 1))
            result[f] = now + rate_ref[f] * (east + west + north + south - 4.0 * now)
        copy = pltpu.make_async_copy(group(result, g), group(out_hbm, g), out_sem.at[g])
        copy.start()
        outs.append(copy)

    for copy in a2a + slabs + edges:
        copy.wait_send()
    for copy in outs:
        copy.wait()


def per_device(
    child_fields, row_weights, col_weights, nest_offsets, priority, parent_old, smooth_rate
):
    planes, crow, ccols = child_fields.shape[1:]
    prd = row_weights.shape[0]
    _, cols, rows = parent_old.shape
    tiles, nests = lax.axis_size("tile"), lax.axis_size("nest")
    per = LANES // cols
    groups = planes // per
    nrows = prd * tiles
    smem = pl.BlockSpec(memory_space=pltpu.SMEM)
    vmem = pl.BlockSpec(memory_space=pltpu.VMEM)
    hbm = pl.BlockSpec(memory_space=pl.ANY)
    dma = pltpu.SemaphoreType.DMA
    return pl.pallas_call(
        functools.partial(kernel, tiles, nests),
        out_shape=jax.ShapeDtypeStruct(parent_old.shape, F32),
        in_specs=[smem, smem, vmem, vmem, hbm, hbm, hbm],
        out_specs=hbm,
        scratch_shapes=[
            pltpu.VMEM((planes, crow, ccols), F32),
            pltpu.VMEM(col_weights.shape, F32),
            pltpu.VMEM((planes, cols, rows), F32),
            pltpu.VMEM((groups, tiles, prd, LANES), F32),
            pltpu.VMEM((nests, groups, nrows, LANES), F32),
            pltpu.VMEM((groups, 2, per, rows), F32),
            pltpu.VMEM((groups, 2, per, rows), F32),
            pltpu.VMEM((groups, 2, cols, LANES), F32),
            pltpu.VMEM((groups, 2, cols, LANES), F32),
            pltpu.VMEM((planes, cols, rows), F32),
            dma((groups,)),
            dma,
            dma,
            dma((groups,)),
            dma((groups, tiles)),
            dma((groups, tiles)),
            dma((groups, max(nests - 1, 3))),
            dma((groups, nests)),
            dma((groups, 4)),
            dma((groups, 4)),
        ],
        compiler_params=pltpu.CompilerParams(
            collective_id=0, has_side_effects=True, vmem_limit_bytes=60 * 1024 * 1024
        ),
    )(nest_offsets, smooth_rate, row_weights, priority, child_fields, col_weights, parent_old)


def solution(mesh):
    return jax.shard_map(
        per_device,
        mesh=mesh,
        in_specs=(
            P("nest", None, "tile", None),
            P(),
            P(),
            P(),
            P("tile", "nest"),
            P(None, "tile", "nest"),
            P(),
        ),
        out_specs=P(None, "tile", "nest"),
        check_vma=False,
    )
```

```python
import functools

import jax
import jax.numpy as jnp
from jax import lax
from jax.experimental import pallas as pl
from jax.experimental.pallas import tpu as pltpu
from jax.sharding import PartitionSpec as P

MESH = pl.DeviceIdType.MESH
LANES = 128
F32 = jnp.float32
BF16 = jnp.bfloat16


def split(value):
    high = value.astype(BF16)
    return high, (value - high.astype(F32)).astype(BF16)


def dot(a, b):
    return jnp.dot(a, b, preferred_element_type=F32)


def dot3(a, b):
    (ah, al), (bh, bl) = a, b
    return dot(ah, bh) + (dot(ah, bl) + dot(al, bh))


def remote(src, dst, send_sem, recv_sem, where):
    return pltpu.make_async_remote_copy(
        src_ref=src,
        dst_ref=dst,
        send_sem=send_sem,
        recv_sem=recv_sem,
        device_id=where,
        device_id_type=MESH,
    )


def kernel(
    tiles,
    nests,
    offs_ref,
    rate_ref,
    rw_ref,
    prio_ref,
    child_hbm,
    cw_hbm,
    parent_hbm,
    out_hbm,
    child,
    cw,
    merged,
    pieces,
    strips,
    ew_out,
    ew_in,
    ns_out,
    ns_in,
    result,
    child_sem,
    cw_sem,
    parent_sem,
    out_sem,
    a2a_send,
    a2a_recv,
    slab_send,
    slab_recv,
    edge_send,
    edge_recv,
):
    planes, crow, _ = child.shape
    prd = rw_ref.shape[0]
    cols, rows = prio_ref.shape
    per = LANES // cols
    groups = planes // per
    nrows = prd * tiles
    me_n, me_t = lax.axis_index("nest"), lax.axis_index("tile")

    def group(ref, g):
        return ref.at[pl.ds(g * per, per)]

    child_in = [
        pltpu.make_async_copy(group(child_hbm.at[0], g), group(child, g), child_sem.at[g])
        for g in range(groups)
    ]
    cw_in = pltpu.make_async_copy(cw_hbm, cw, cw_sem)
    parent_in = pltpu.make_async_copy(parent_hbm, merged, parent_sem)
    child_in[0].start()
    cw_in.start()
    for g in range(1, groups):
        child_in[g].start()
    parent_in.start()

    barrier = pltpu.get_barrier_semaphore()
    for d in range(1, tiles):
        pl.semaphore_signal(
            barrier, inc=1, device_id={"tile": lax.rem(me_t + d, tiles)}, device_id_type=MESH
        )
    for d in range(1, nests):
        pl.semaphore_signal(
            barrier, inc=1, device_id={"nest": lax.rem(me_n + d, nests)}, device_id_type=MESH
        )

    rw = rw_ref[...]
    spread_rows = lax.broadcasted_iota(jnp.int32, (per * crow, crow), 0)
    spread_cols = lax.broadcasted_iota(jnp.int32, (per * crow, crow), 1)
    spread = jnp.where(lax.rem(spread_rows, crow) == spread_cols, 1.0, 0.0).astype(BF16)
    wide_r = lax.broadcasted_iota(jnp.int32, (per * prd, per * crow), 0)
    wide_c = lax.broadcasted_iota(jnp.int32, (per * prd, per * crow), 1)
    diagonal = wide_r // prd == wide_c // crow
    block_rw = []
    for part in split(rw):
        line = lax.dot_general(
            part, spread, (((1,), (1,)), ((), ())), preferred_element_type=F32
        )
        line = jnp.concatenate([line] * per, axis=0)
        block_rw.append(jnp.where(diagonal, line, 0.0).astype(BF16))

    lane_group = lax.broadcasted_iota(jnp.int32, (prd, LANES), 1) // cols
    left = jnp.int32(0)
    for n in range(nests):
        left = jnp.where(me_n == n, offs_ref[1, n], left)

    a2a, cw_split = [], []

    def restrict(g):
        child_in[g].wait()
        block = child[g * per : (g + 1) * per].reshape(per * crow, child.shape[2])
        thinned = dot3(block_rw, split(block))
        if not cw_split:
            cw_in.wait()
            cw_split.extend(split(cw[...]))
        restricted = dot3(split(thinned), cw_split)
        restricted = pltpu.roll(restricted, left, 1)
        for t in range(tiles):
            base, off = (t * cols) // LANES * LANES, (t * cols) % LANES
            piece = None
            for j in range(per):
                part = restricted[j * prd : (j + 1) * prd, base : base + LANES]
                shift = (j * cols - off) % LANES
                if shift:
                    part = pltpu.roll(part, shift, 1)
                piece = part if j == 0 else jnp.where(lane_group == j, part, piece)
            pieces[g, t] = piece
        here = pl.ds(pl.multiple_of(me_t * prd, prd), prd)
        strips[me_n, g, here, :] = pieces[g, me_t]
        if g == 0:
            pl.semaphore_wait(barrier, tiles + nests - 2)
        for d in range(1, tiles):
            t = lax.rem(me_t + d, tiles)
            copy = remote(
                pieces.at[g, t],
                strips.at[me_n, g, here, :],
                a2a_send.at[g, t],
                a2a_recv.at[g, me_t],
                {"tile": t},
            )
            copy.start()
            a2a.append(copy)

    slabs = []

    def send_slab(owner, g, to, slot):
        copy = remote(
            strips.at[owner, g],
            strips.at[owner, g],
            slab_send.at[g, slot],
            slab_recv.at[g, owner],
            {"nest": to},
        )
        copy.start()
        slabs.append(copy)

    def wait_slab(owner, g):
        remote(
            strips.at[owner, g],
            strips.at[owner, g],
            slab_send.at[g, 0],
            slab_recv.at[g, owner],
            {"nest": owner},
        ).wait_recv()

    def flip(mask):
        if mask == 1:
            return me_n + 1 - 2 * lax.rem(me_n, 2)
        if mask == 2:
            return lax.rem(me_n + 2, 4)
        return 3 - me_n

    relayed = nests == 4

    def relay(g):
        if not relayed:
            return
        first, second = (flip(1), flip(2)) if g % 2 == 0 else (flip(2), flip(1))
        wait_slab(first, g)
        send_slab(first, g, second, 2)

    def forward(g):
        for d in range(1, tiles):
            t = lax.rem(me_t + d, tiles)
            there = pl.ds(pl.multiple_of(t * prd, prd), prd)
            remote(
                pieces.at[g, t],
                strips.at[me_n, g, there, :],
                a2a_send.at[g, t],
                a2a_recv.at[g, t],
                {"tile": t},
            ).wait_recv()
        if relayed:
            send_slab(me_n, g, flip(1 + g % 2), 0)
            send_slab(me_n, g, flip(2 - g % 2), 1)
        else:
            for d in range(1, nests):
                send_slab(me_n, g, lax.rem(me_n + d, nests), d - 1)

    own_start = me_n * rows
    place_r = lax.rem(lax.broadcasted_iota(jnp.int32, (2 * nrows, rows), 0), nrows)
    place_c = lax.broadcasted_iota(jnp.int32, (2 * nrows, rows), 1)
    prio = prio_ref[...]
    west_t, east_t = lax.rem(me_t + tiles - 1, tiles), lax.rem(me_t + 1, tiles)
    low_n, high_n = lax.rem(me_n + nests - 1, nests), lax.rem(me_n + 1, nests)
    lane = lax.broadcasted_iota(jnp.int32, (cols, LANES), 1)
    places = []
    for n in range(nests):
        hit = place_c - place_r == offs_ref[0, n] - own_start
        places.append(jnp.where(hit, 1.0, 0.0).astype(BF16))

    edges = {}

    def merge(g):
        if g == 0:
            parent_in.wait()
        if relayed:
            first, second = (flip(1), flip(2)) if g % 2 == 0 else (flip(2), flip(1))
            wait_slab(second, g)
            wait_slab(flip(3), g)
        else:
            for d in range(1, nests):
                wait_slab(lax.rem(me_n + d, nests), g)
        now = merged[g * per : (g + 1) * per]
        for n in range(nests):
            slab = jnp.concatenate(split(strips[n, g]), axis=0)
            placed = lax.dot_general(
                slab, places[n], (((0,), (0,)), ((), ())), preferred_element_type=F32
            )
            now = jnp.where((prio == n)[None], placed.reshape(per, cols, rows), now)
        merged[g * per : (g + 1) * per] = now
        low = jnp.zeros((cols, LANES), F32)
        high = jnp.zeros((cols, LANES), F32)
        for j in range(per):
            low = jnp.where(lane == j, now[j, :, :1], low)
            high = jnp.where(lane == j, now[j, :, rows - 1 :], high)
            ew_out[g, 0, j : j + 1] = now[j, :1]
            ew_out[g, 1, j : j + 1] = now[j, cols - 1 :]
        ns_out[g, 0] = low
        ns_out[g, 1] = high
        for side, (source, target, where) in enumerate(
            (
                (ew_out.at[g, 0], ew_in.at[g, 0], {"tile": west_t}),
                (ew_out.at[g, 1], ew_in.at[g, 1], {"tile": east_t}),
                (ns_out.at[g, 0], ns_in.at[g, 0], {"nest": low_n}),
                (ns_out.at[g, 1], ns_in.at[g, 1], {"nest": high_n}),
            )
        ):
            copy = remote(source, target, edge_send.at[g, side], edge_recv.at[g, side], where)
            copy.start()
            edges[g, side] = copy

    row_lane = lax.broadcasted_iota(jnp.int32, (cols, rows), 1)
    outs = []

    def finish(g):
        for side in range(4):
            edges[g, side].wait_recv()
        smoothed = []
        for j in range(per):
            f = g * per + j
            now = merged[f]
            east = jnp.concatenate([now[1:], ew_in[g, 0, j : j + 1]], axis=0)
            west = jnp.concatenate([ew_in[g, 1, j : j + 1], now[:-1]], axis=0)
            above = jnp.where(me_n == nests - 1, now[:, rows - 1 :], ns_in[g, 0, :, j : j + 1])
            below = jnp.where(me_n == 0, now[:, :1], ns_in[g, 1, :, j : j + 1])
            north = jnp.where(row_lane == rows - 1, above, pltpu.roll(now, rows - 1, 1))
            south = jnp.where(row_lane == 0, below, pltpu.roll(now, 1, 1))
            smoothed.append(now + rate_ref[f] * (east + west + north + south - 4.0 * now))
        for j in range(per):
            result[g * per + j] = smoothed[j]
        copy = pltpu.make_async_copy(group(result, g), group(out_hbm, g), out_sem.at[g])
        copy.start()
        outs.append(copy)

    lags = ((restrict, 0), (forward, 1), (relay, 2), (merge, 3), (finish, 5))
    for step in range(groups + 5):
        for stage, lag in lags:
            if 0 <= step - lag < groups:
                stage(step - lag)

    for copy in a2a + slabs + list(edges.values()):
        copy.wait_send()
    for copy in outs:
        copy.wait()


def per_device(
    child_fields, row_weights, col_weights, nest_offsets, priority, parent_old, smooth_rate
):
    planes, crow, ccols = child_fields.shape[1:]
    prd = row_weights.shape[0]
    _, cols, rows = parent_old.shape
    tiles, nests = lax.axis_size("tile"), lax.axis_size("nest")
    per = LANES // cols
    groups = planes // per
    nrows = prd * tiles
    smem = pl.BlockSpec(memory_space=pltpu.SMEM)
    vmem = pl.BlockSpec(memory_space=pltpu.VMEM)
    hbm = pl.BlockSpec(memory_space=pl.ANY)
    dma = pltpu.SemaphoreType.DMA
    return pl.pallas_call(
        functools.partial(kernel, tiles, nests),
        out_shape=jax.ShapeDtypeStruct(parent_old.shape, F32),
        in_specs=[smem, smem, vmem, vmem, hbm, hbm, hbm],
        out_specs=hbm,
        scratch_shapes=[
            pltpu.VMEM((planes, crow, ccols), F32),
            pltpu.VMEM(col_weights.shape, F32),
            pltpu.VMEM((planes, cols, rows), F32),
            pltpu.VMEM((groups, tiles, prd, LANES), F32),
            pltpu.VMEM((nests, groups, nrows, LANES), F32),
            pltpu.VMEM((groups, 2, per, rows), F32),
            pltpu.VMEM((groups, 2, per, rows), F32),
            pltpu.VMEM((groups, 2, cols, LANES), F32),
            pltpu.VMEM((groups, 2, cols, LANES), F32),
            pltpu.VMEM((planes, cols, rows), F32),
            dma((groups,)),
            dma,
            dma,
            dma((groups,)),
            dma((groups, tiles)),
            dma((groups, tiles)),
            dma((groups, max(nests - 1, 3))),
            dma((groups, nests)),
            dma((groups, 4)),
            dma((groups, 4)),
        ],
        compiler_params=pltpu.CompilerParams(
            collective_id=0, has_side_effects=True, vmem_limit_bytes=60 * 1024 * 1024
        ),
    )(nest_offsets.T, smooth_rate, row_weights, priority, child_fields, col_weights, parent_old)


def solution(mesh):
    return jax.shard_map(
        per_device,
        mesh=mesh,
        in_specs=(
            P("nest", None, "tile", None),
            P(),
            P(),
            P(),
            P("tile", "nest"),
            P(None, "tile", "nest"),
            P(),
        ),
        out_specs=P(None, "tile", "nest"),
        check_vma=False,
    )
```

```python
import functools

import jax
import jax.numpy as jnp
from jax import lax
from jax.experimental import pallas as pl
from jax.experimental.pallas import tpu as pltpu
from jax.sharding import PartitionSpec as P

MESH = pl.DeviceIdType.MESH
LANES = 128
F32 = jnp.float32
BF16 = jnp.bfloat16


def split(value):
    high = value.astype(BF16)
    return high, (value - high.astype(F32)).astype(BF16)


def dot(a, b):
    return jnp.dot(a, b, preferred_element_type=F32)


def dot3(a, b):
    (ah, al), (bh, bl) = a, b
    return dot(ah, bh) + (dot(ah, bl) + dot(al, bh))


def remote(src, dst, send_sem, recv_sem, where):
    return pltpu.make_async_remote_copy(
        src_ref=src,
        dst_ref=dst,
        send_sem=send_sem,
        recv_sem=recv_sem,
        device_id=where,
        device_id_type=MESH,
    )


def order(groups):
    yield "R", 0
    for g in range(1, groups):
        yield "R", g
        if g == 1:
            yield "S", 0
        yield "S", g
    if groups == 1:
        yield "S", 0
    for stage in "FME":
        yield from ((stage, g) for g in range(groups))


def kernel(
    tiles,
    nests,
    offs_ref,
    rate_ref,
    rw_hbm,
    prio_hbm,
    child_hbm,
    cw_hbm,
    parent_hbm,
    out_hbm,
    rw_ref,
    prio_ref,
    child,
    cw,
    merged,
    pieces,
    strips,
    ew_out,
    ew_in,
    ns_out,
    ns_in,
    result,
    small_sem,
    child_sem,
    cw_sem,
    parent_sem,
    out_sem,
    a2a_send,
    a2a_recv,
    slab_send,
    slab_recv,
    edge_send,
    edge_recv,
):
    planes, crow, _ = child.shape
    prd = rw_ref.shape[0]
    cols, rows = prio_ref.shape
    per = LANES // cols
    groups = planes // per
    nrows = prd * tiles
    me_n, me_t = lax.axis_index("nest"), lax.axis_index("tile")

    def group(ref, g):
        return ref.at[pl.ds(g * per, per)]

    child_in = [
        pltpu.make_async_copy(group(child_hbm.at[0], g), group(child, g), child_sem.at[g])
        for g in range(groups)
    ]
    cw_in = pltpu.make_async_copy(cw_hbm, cw, cw_sem)
    parent_in = pltpu.make_async_copy(parent_hbm, merged, parent_sem)
    barrier = pltpu.get_barrier_semaphore()
    for d in range(1, tiles):
        pl.semaphore_signal(
            barrier, inc=1, device_id={"tile": lax.rem(me_t + d, tiles)}, device_id_type=MESH
        )
    for d in range(1, nests):
        pl.semaphore_signal(
            barrier, inc=1, device_id={"nest": lax.rem(me_n + d, nests)}, device_id_type=MESH
        )
    rw_in = pltpu.make_async_copy(rw_hbm, rw_ref, small_sem.at[0])
    prio_in = pltpu.make_async_copy(prio_hbm, prio_ref, small_sem.at[1])
    rw_in.start()
    child_in[0].start()
    cw_in.start()
    for g in range(1, groups):
        child_in[g].start()
    prio_in.start()
    parent_in.start()

    rw_in.wait()
    rw = rw_ref[...]
    spread_rows = lax.broadcasted_iota(jnp.int32, (per * crow, crow), 0)
    spread_cols = lax.broadcasted_iota(jnp.int32, (per * crow, crow), 1)
    spread = jnp.where(lax.rem(spread_rows, crow) == spread_cols, 1.0, 0.0).astype(BF16)
    wide_r = lax.broadcasted_iota(jnp.int32, (per * prd, per * crow), 0)
    wide_c = lax.broadcasted_iota(jnp.int32, (per * prd, per * crow), 1)
    diagonal = wide_r // prd == wide_c // crow
    block_rw = []
    for part in split(rw):
        line = lax.dot_general(
            part, spread, (((1,), (1,)), ((), ())), preferred_element_type=F32
        )
        line = jnp.concatenate([line] * per, axis=0)
        block_rw.append(jnp.where(diagonal, line, 0.0).astype(BF16))

    lane_group = lax.broadcasted_iota(jnp.int32, (prd, LANES), 1) // cols
    left = jnp.int32(0)
    for n in range(nests):
        left = jnp.where(me_n == n, offs_ref[1, n], left)

    a2a, cw_split = [], []

    here = pl.ds(pl.multiple_of(me_t * prd, prd), prd)

    def restrict(g):
        child_in[g].wait()
        block = child[g * per : (g + 1) * per].reshape(per * crow, child.shape[2])
        thinned = dot3(block_rw, split(block))
        if not cw_split:
            cw_in.wait()
            cw_split.extend(split(cw[...]))
        restricted = dot3(split(thinned), cw_split)
        restricted = pltpu.roll(restricted, left, 1)
        for t in range(tiles):
            base, off = (t * cols) // LANES * LANES, (t * cols) % LANES
            piece = None
            for j in range(per):
                part = restricted[j * prd : (j + 1) * prd, base : base + LANES]
                shift = (j * cols - off) % LANES
                if shift:
                    part = pltpu.roll(part, shift, 1)
                piece = part if j == 0 else jnp.where(lane_group == j, part, piece)
            pieces[g, t] = piece
        strips[me_n, g, here, :] = pieces[g, me_t]

    def send(g):
        if g == 0:
            pl.semaphore_wait(barrier, tiles + nests - 2)
        for d in range(1, tiles):
            t = lax.rem(me_t + d, tiles)
            copy = remote(
                pieces.at[g, t],
                strips.at[me_n, g, here, :],
                a2a_send.at[g, t],
                a2a_recv.at[g, me_t],
                {"tile": t},
            )
            copy.start()
            a2a.append(copy)

    slabs = []

    def send_slab(owner, g, to, slot):
        copy = remote(
            strips.at[owner, g],
            strips.at[owner, g],
            slab_send.at[g, slot],
            slab_recv.at[g, owner],
            {"nest": to},
        )
        copy.start()
        slabs.append(copy)

    def wait_slab(owner, g):
        remote(
            strips.at[owner, g],
            strips.at[owner, g],
            slab_send.at[g, 0],
            slab_recv.at[g, owner],
            {"nest": owner},
        ).wait_recv()

    def forward(g):
        for d in range(1, tiles):
            t = lax.rem(me_t + d, tiles)
            there = pl.ds(pl.multiple_of(t * prd, prd), prd)
            remote(
                pieces.at[g, t],
                strips.at[me_n, g, there, :],
                a2a_send.at[g, t],
                a2a_recv.at[g, t],
                {"tile": t},
            ).wait_recv()
        for d in range(1, nests):
            send_slab(me_n, g, lax.rem(me_n + d, nests), d - 1)

    own_start = me_n * rows
    place_r = lax.rem(lax.broadcasted_iota(jnp.int32, (2 * nrows, rows), 0), nrows)
    place_c = lax.broadcasted_iota(jnp.int32, (2 * nrows, rows), 1)
    prio_in.wait()
    prio = prio_ref[...]
    west_t, east_t = lax.rem(me_t + tiles - 1, tiles), lax.rem(me_t + 1, tiles)
    low_n, high_n = lax.rem(me_n + nests - 1, nests), lax.rem(me_n + 1, nests)
    lane = lax.broadcasted_iota(jnp.int32, (cols, LANES), 1)
    places = []
    for n in range(nests):
        hit = place_c - place_r == offs_ref[0, n] - own_start
        places.append(jnp.where(hit, 1.0, 0.0).astype(BF16))

    edges = {}

    def merge(g):
        if g == 0:
            parent_in.wait()
        for d in range(1, nests):
            wait_slab(lax.rem(me_n + d, nests), g)
        now = merged[g * per : (g + 1) * per]
        for n in range(nests):
            slab = jnp.concatenate(split(strips[n, g]), axis=0)
            placed = lax.dot_general(
                slab, places[n], (((0,), (0,)), ((), ())), preferred_element_type=F32
            )
            now = jnp.where((prio == n)[None], placed.reshape(per, cols, rows), now)
        merged[g * per : (g + 1) * per] = now
        low = jnp.zeros((cols, LANES), F32)
        high = jnp.zeros((cols, LANES), F32)
        for j in range(per):
            low = jnp.where(lane == j, now[j, :, :1], low)
            high = jnp.where(lane == j, now[j, :, rows - 1 :], high)
            ew_out[g, 0, j : j + 1] = now[j, :1]
            ew_out[g, 1, j : j + 1] = now[j, cols - 1 :]
        ns_out[g, 0] = low
        ns_out[g, 1] = high
        for side, (source, target, where) in enumerate(
            (
                (ew_out.at[g, 0], ew_in.at[g, 0], {"tile": west_t}),
                (ew_out.at[g, 1], ew_in.at[g, 1], {"tile": east_t}),
                (ns_out.at[g, 0], ns_in.at[g, 0], {"nest": low_n}),
                (ns_out.at[g, 1], ns_in.at[g, 1], {"nest": high_n}),
            )
        ):
            copy = remote(source, target, edge_send.at[g, side], edge_recv.at[g, side], where)
            copy.start()
            edges[g, side] = copy

    row_lane = lax.broadcasted_iota(jnp.int32, (cols, rows), 1)
    outs = []

    def finish(g):
        for side in range(4):
            edges[g, side].wait_recv()
        smoothed = []
        for j in range(per):
            f = g * per + j
            now = merged[f]
            east = jnp.concatenate([now[1:], ew_in[g, 0, j : j + 1]], axis=0)
            west = jnp.concatenate([ew_in[g, 1, j : j + 1], now[:-1]], axis=0)
            above = jnp.where(me_n == nests - 1, now[:, rows - 1 :], ns_in[g, 0, :, j : j + 1])
            below = jnp.where(me_n == 0, now[:, :1], ns_in[g, 1, :, j : j + 1])
            north = jnp.where(row_lane == rows - 1, above, pltpu.roll(now, rows - 1, 1))
            south = jnp.where(row_lane == 0, below, pltpu.roll(now, 1, 1))
            smoothed.append(now + rate_ref[f] * (east + west + north + south - 4.0 * now))
        for j in range(per):
            result[g * per + j] = smoothed[j]
        copy = pltpu.make_async_copy(group(result, g), group(out_hbm, g), out_sem.at[g])
        copy.start()
        outs.append(copy)

    stages = {"R": restrict, "S": send, "F": forward, "M": merge, "E": finish}
    for step in order(groups):
        stages[step[0]](step[1])

    for copy in a2a + slabs + list(edges.values()):
        copy.wait_send()
    for copy in outs:
        copy.wait()


def per_device(
    child_fields, row_weights, col_weights, nest_offsets, priority, parent_old, smooth_rate
):
    planes, crow, ccols = child_fields.shape[1:]
    prd = row_weights.shape[0]
    _, cols, rows = parent_old.shape
    tiles, nests = lax.axis_size("tile"), lax.axis_size("nest")
    per = LANES // cols
    groups = planes // per
    nrows = prd * tiles
    smem = pl.BlockSpec(memory_space=pltpu.SMEM)
    hbm = pl.BlockSpec(memory_space=pl.ANY)
    dma = pltpu.SemaphoreType.DMA
    return pl.pallas_call(
        functools.partial(kernel, tiles, nests),
        out_shape=jax.ShapeDtypeStruct(parent_old.shape, F32),
        in_specs=[smem, smem] + [hbm] * 5,
        out_specs=hbm,
        scratch_shapes=[
            pltpu.VMEM(row_weights.shape, F32),
            pltpu.VMEM((cols, rows), jnp.int32),
            pltpu.VMEM((planes, crow, ccols), F32),
            pltpu.VMEM(col_weights.shape, F32),
            pltpu.VMEM((planes, cols, rows), F32),
            pltpu.VMEM((groups, tiles, prd, LANES), F32),
            pltpu.VMEM((nests, groups, nrows, LANES), F32),
            pltpu.VMEM((groups, 2, per, rows), F32),
            pltpu.VMEM((groups, 2, per, rows), F32),
            pltpu.VMEM((groups, 2, cols, LANES), F32),
            pltpu.VMEM((groups, 2, cols, LANES), F32),
            pltpu.VMEM((planes, cols, rows), F32),
            dma((2,)),
            dma((groups,)),
            dma,
            dma,
            dma((groups,)),
            dma((groups, tiles)),
            dma((groups, tiles)),
            dma((groups, nests - 1)),
            dma((groups, nests)),
            dma((groups, 4)),
            dma((groups, 4)),
        ],
        compiler_params=pltpu.CompilerParams(
            collective_id=0, has_side_effects=True, vmem_limit_bytes=60 * 2**20
        ),
    )(nest_offsets.T, smooth_rate, row_weights, priority, child_fields, col_weights, parent_old)


def solution(mesh):
    return jax.shard_map(
        per_device,
        mesh=mesh,
        in_specs=(
            P("nest", None, "tile", None),
            P(),
            P(),
            P(),
            P("tile", "nest"),
            P(None, "tile", "nest"),
            P(),
        ),
        out_specs=P(None, "tile", "nest"),
        check_vma=False,
    )
```

```python
import functools

import jax
import jax.numpy as jnp
from jax import lax
from jax.experimental import pallas as pl
from jax.experimental.pallas import tpu as pltpu
from jax.sharding import PartitionSpec as P

MESH = pl.DeviceIdType.MESH
LANES = 128
F32 = jnp.float32
BF16 = jnp.bfloat16


def split(value):
    high = value.astype(BF16)
    return high, (value - high.astype(F32)).astype(BF16)


def dot(a, b):
    return jnp.dot(a, b, preferred_element_type=F32)


def dot3(a, b):
    (ah, al), (bh, bl) = a, b
    return dot(ah, bh) + (dot(ah, bl) + dot(al, bh))


def remote(src, dst, send_sem, recv_sem, where):
    return pltpu.make_async_remote_copy(
        src_ref=src,
        dst_ref=dst,
        send_sem=send_sem,
        recv_sem=recv_sem,
        device_id=where,
        device_id_type=MESH,
    )


def order(groups):
    yield "R", 0
    for g in range(1, groups):
        yield "R", g
        if g == 1:
            yield "S", 0
        yield "S", g
    if groups == 1:
        yield "S", 0
    for stage in "FME":
        yield from ((stage, g) for g in range(groups))


def kernel(
    tiles,
    nests,
    offs_ref,
    rate_ref,
    rw_hbm,
    prio_hbm,
    child_hbm,
    cw_hbm,
    parent_hbm,
    result,
    rw_ref,
    prio_ref,
    child,
    cw,
    merged,
    pieces,
    strips,
    ew_out,
    ew_in,
    ns_out,
    ns_in,
    small_sem,
    child_sem,
    cw_sem,
    parent_sem,
    a2a_send,
    a2a_recv,
    slab_send,
    slab_recv,
    edge_send,
    edge_recv,
):
    planes, crow, _ = child.shape
    prd = rw_ref.shape[0]
    cols, rows = prio_ref.shape
    per = LANES // cols
    groups = planes // per
    nrows = prd * tiles
    me_n, me_t = lax.axis_index("nest"), lax.axis_index("tile")

    def group(ref, g):
        return ref.at[pl.ds(g * per, per)]

    child_in = [
        pltpu.make_async_copy(group(child_hbm.at[0], g), group(child, g), child_sem.at[g])
        for g in range(groups)
    ]
    cw_in = pltpu.make_async_copy(cw_hbm, cw, cw_sem)
    parent_in = pltpu.make_async_copy(parent_hbm, merged, parent_sem)
    barrier = pltpu.get_barrier_semaphore()
    for d in range(1, tiles):
        pl.semaphore_signal(
            barrier, inc=1, device_id={"tile": lax.rem(me_t + d, tiles)}, device_id_type=MESH
        )
    for d in range(1, nests):
        pl.semaphore_signal(
            barrier, inc=1, device_id={"nest": lax.rem(me_n + d, nests)}, device_id_type=MESH
        )
    rw_in = pltpu.make_async_copy(rw_hbm, rw_ref, small_sem.at[0])
    prio_in = pltpu.make_async_copy(prio_hbm, prio_ref, small_sem.at[1])
    rw_in.start()
    child_in[0].start()
    cw_in.start()
    for g in range(1, groups):
        child_in[g].start()
    prio_in.start()
    parent_in.start()

    rw_in.wait()
    rw = rw_ref[...]
    spread_rows = lax.broadcasted_iota(jnp.int32, (per * crow, crow), 0)
    spread_cols = lax.broadcasted_iota(jnp.int32, (per * crow, crow), 1)
    spread = jnp.where(lax.rem(spread_rows, crow) == spread_cols, 1.0, 0.0).astype(BF16)
    wide_r = lax.broadcasted_iota(jnp.int32, (per * prd, per * crow), 0)
    wide_c = lax.broadcasted_iota(jnp.int32, (per * prd, per * crow), 1)
    diagonal = wide_r // prd == wide_c // crow
    block_rw = []
    for part in split(rw):
        line = lax.dot_general(
            part, spread, (((1,), (1,)), ((), ())), preferred_element_type=F32
        )
        line = jnp.concatenate([line] * per, axis=0)
        block_rw.append(jnp.where(diagonal, line, 0.0).astype(BF16))

    lane_group = lax.broadcasted_iota(jnp.int32, (prd, LANES), 1) // cols
    left = jnp.int32(0)
    for n in range(nests):
        left = jnp.where(me_n == n, offs_ref[1, n], left)

    a2a, cw_split = [], []

    here = pl.ds(pl.multiple_of(me_t * prd, prd), prd)

    def restrict(g):
        child_in[g].wait()
        block = child[g * per : (g + 1) * per].reshape(per * crow, child.shape[2])
        thinned = dot3(block_rw, split(block))
        if not cw_split:
            cw_in.wait()
            cw_split.extend(split(cw[...]))
        restricted = dot3(split(thinned), cw_split)
        restricted = pltpu.roll(restricted, left, 1)
        for t in range(tiles):
            base, off = (t * cols) // LANES * LANES, (t * cols) % LANES
            piece = None
            for j in range(per):
                part = restricted[j * prd : (j + 1) * prd, base : base + LANES]
                shift = (j * cols - off) % LANES
                if shift:
                    part = pltpu.roll(part, shift, 1)
                piece = part if j == 0 else jnp.where(lane_group == j, part, piece)
            pieces[g, t] = piece
        strips[me_n, g, here, :] = pieces[g, me_t]

    def send(g):
        if g == 0:
            pl.semaphore_wait(barrier, tiles + nests - 2)
        for d in range(1, tiles):
            t = lax.rem(me_t + d, tiles)
            copy = remote(
                pieces.at[g, t],
                strips.at[me_n, g, here, :],
                a2a_send.at[g, t],
                a2a_recv.at[g, me_t],
                {"tile": t},
            )
            copy.start()
            a2a.append(copy)

    slabs = []

    def send_slab(owner, g, to, slot):
        copy = remote(
            strips.at[owner, g],
            strips.at[owner, g],
            slab_send.at[g, slot],
            slab_recv.at[g, owner],
            {"nest": to},
        )
        copy.start()
        slabs.append(copy)

    def wait_slab(owner, g):
        remote(
            strips.at[owner, g],
            strips.at[owner, g],
            slab_send.at[g, 0],
            slab_recv.at[g, owner],
            {"nest": owner},
        ).wait_recv()

    def forward(g):
        for d in range(1, tiles):
            t = lax.rem(me_t + d, tiles)
            there = pl.ds(pl.multiple_of(t * prd, prd), prd)
            remote(
                pieces.at[g, t],
                strips.at[me_n, g, there, :],
                a2a_send.at[g, t],
                a2a_recv.at[g, t],
                {"tile": t},
            ).wait_recv()
        for d in range(1, nests):
            send_slab(me_n, g, lax.rem(me_n + d, nests), d - 1)

    own_start = me_n * rows
    place_r = lax.rem(lax.broadcasted_iota(jnp.int32, (2 * nrows, rows), 0), nrows)
    place_c = lax.broadcasted_iota(jnp.int32, (2 * nrows, rows), 1)
    prio_in.wait()
    prio = prio_ref[...]
    west_t, east_t = lax.rem(me_t + tiles - 1, tiles), lax.rem(me_t + 1, tiles)
    low_n, high_n = lax.rem(me_n + nests - 1, nests), lax.rem(me_n + 1, nests)
    lane = lax.broadcasted_iota(jnp.int32, (cols, LANES), 1)
    places = []
    for n in range(nests):
        hit = place_c - place_r == offs_ref[0, n] - own_start
        places.append(jnp.where(hit, 1.0, 0.0).astype(BF16))

    edges = {}

    def merge(g):
        if g == 0:
            parent_in.wait()
        for d in range(1, nests):
            wait_slab(lax.rem(me_n + d, nests), g)
        now = merged[g * per : (g + 1) * per]
        for n in range(nests):
            slab = jnp.concatenate(split(strips[n, g]), axis=0)
            placed = lax.dot_general(
                slab, places[n], (((0,), (0,)), ((), ())), preferred_element_type=F32
            )
            now = jnp.where((prio == n)[None], placed.reshape(per, cols, rows), now)
        merged[g * per : (g + 1) * per] = now
        low = jnp.zeros((cols, LANES), F32)
        high = jnp.zeros((cols, LANES), F32)
        for j in range(per):
            low = jnp.where(lane == j, now[j, :, :1], low)
            high = jnp.where(lane == j, now[j, :, rows - 1 :], high)
            ew_out[g, 0, j : j + 1] = now[j, :1]
            ew_out[g, 1, j : j + 1] = now[j, cols - 1 :]
        ns_out[g, 0] = low
        ns_out[g, 1] = high
        for side, (source, target, where) in enumerate(
            (
                (ew_out.at[g, 0], ew_in.at[g, 0], {"tile": west_t}),
                (ew_out.at[g, 1], ew_in.at[g, 1], {"tile": east_t}),
                (ns_out.at[g, 0], ns_in.at[g, 0], {"nest": low_n}),
                (ns_out.at[g, 1], ns_in.at[g, 1], {"nest": high_n}),
            )
        ):
            copy = remote(source, target, edge_send.at[g, side], edge_recv.at[g, side], where)
            copy.start()
            edges[g, side] = copy

    row_lane = lax.broadcasted_iota(jnp.int32, (cols, rows), 1)
    def finish(g):
        for side in range(4):
            edges[g, side].wait_recv()
        smoothed = []
        for j in range(per):
            f = g * per + j
            now = merged[f]
            east = jnp.concatenate([now[1:], ew_in[g, 0, j : j + 1]], axis=0)
            west = jnp.concatenate([ew_in[g, 1, j : j + 1], now[:-1]], axis=0)
            above = jnp.where(me_n == nests - 1, now[:, rows - 1 :], ns_in[g, 0, :, j : j + 1])
            below = jnp.where(me_n == 0, now[:, :1], ns_in[g, 1, :, j : j + 1])
            north = jnp.where(row_lane == rows - 1, above, pltpu.roll(now, rows - 1, 1))
            south = jnp.where(row_lane == 0, below, pltpu.roll(now, 1, 1))
            smoothed.append(now + rate_ref[f] * (east + west + north + south - 4.0 * now))
        for j in range(per):
            result[g * per + j] = smoothed[j]

    stages = {"R": restrict, "S": send, "F": forward, "M": merge, "E": finish}
    for step in order(groups):
        stages[step[0]](step[1])

    for copy in a2a + slabs + list(edges.values()):
        copy.wait_send()


def per_device(
    child_fields, row_weights, col_weights, nest_offsets, priority, parent_old, smooth_rate
):
    planes, crow, ccols = child_fields.shape[1:]
    prd = row_weights.shape[0]
    _, cols, rows = parent_old.shape
    tiles, nests = lax.axis_size("tile"), lax.axis_size("nest")
    per = LANES // cols
    groups = planes // per
    nrows = prd * tiles
    smem = pl.BlockSpec(memory_space=pltpu.SMEM)
    hbm = pl.BlockSpec(memory_space=pl.ANY)
    dma = pltpu.SemaphoreType.DMA
    return pl.pallas_call(
        functools.partial(kernel, tiles, nests),
        out_shape=pltpu.VMEM(parent_old.shape, F32),
        in_specs=[smem, smem] + [hbm] * 5,
        out_specs=pl.BlockSpec(memory_space=pltpu.VMEM),
        scratch_shapes=[
            pltpu.VMEM(row_weights.shape, F32),
            pltpu.VMEM((cols, rows), jnp.int32),
            pltpu.VMEM((planes, crow, ccols), F32),
            pltpu.VMEM(col_weights.shape, F32),
            pltpu.VMEM((planes, cols, rows), F32),
            pltpu.VMEM((groups, tiles, prd, LANES), F32),
            pltpu.VMEM((nests, groups, nrows, LANES), F32),
            pltpu.VMEM((groups, 2, per, rows), F32),
            pltpu.VMEM((groups, 2, per, rows), F32),
            pltpu.VMEM((groups, 2, cols, LANES), F32),
            pltpu.VMEM((groups, 2, cols, LANES), F32),
            dma((2,)),
            dma((groups,)),
            dma,
            dma,
            dma((groups, tiles)),
            dma((groups, tiles)),
            dma((groups, nests - 1)),
            dma((groups, nests)),
            dma((groups, 4)),
            dma((groups, 4)),
        ],
        compiler_params=pltpu.CompilerParams(
            collective_id=0, has_side_effects=True, vmem_limit_bytes=60 * 2**20
        ),
    )(nest_offsets.T, smooth_rate, row_weights, priority, child_fields, col_weights, parent_old)


def solution(mesh):
    return jax.shard_map(
        per_device,
        mesh=mesh,
        in_specs=(
            P("nest", None, "tile", None),
            P(),
            P(),
            P(),
            P("tile", "nest"),
            P(None, "tile", "nest"),
            P(),
        ),
        out_specs=P(None, "tile", "nest"),
        check_vma=False,
    )
```
